32 devices in a mesh: layer: 2 (over core), px: 4 (over z), py: 4 (over y, x).
Axes of the slice: x: 2, y: 2, z: 4, core: 2. Of those that a mesh axis runs over, the one named last changes fastest.
Arguments:
- right_side: float32 [8, 512, 4096], P('layer', 'px', 'py'), may hold values from -30 to 30
- row_conduct: float32 [8, 512, 4096], P('layer', 'px', 'py'), may hold values from 0.5 to 2
- column_conduct: float32 [8, 512, 4096], P('layer', 'px', 'py'), may hold values from 0.5 to 2
- via_conduct: float32 [8, 512, 4096], P('layer', 'px', 'py'), may hold values from 0.5 to 4
- via_mask: int32 [8, 512, 4096], P('layer', 'px', 'py'), may hold values 0 or 1
- ground_conduct: float32 [8, 512, 4096], P('layer', 'px', 'py'), may hold values from 0.01 to 0.1
Outputs:
- solution_field: float32 [8, 512, 4096], P('layer', 'px', 'py')
- residual: float32 [8, 512, 4096], P('layer', 'px', 'py')
The draws below stay inside these ranges and needn't reach their ends.
All inputs are finite; a program needn't handle non-finite values. No bound on the sum of `via_mask` on one device may be relied on, other than what follows from the above.
Results may differ from the reference program's by a relative error of at most 0.0001.
Values sent between devices are 32-bit elements; how exact they have to be, the bound alone decides.
A program may use at most 128 MiB of HBM per device.

```python
import math
import jax
import jax.numpy as jnp

ITERS = 2
LAYERS = 8
NX = 512
NY = 4096


def draw_right_side(key, part):
    noise = jax.random.normal(key, (LAYERS, NX, NY), jnp.float32)
    rows = jnp.arange(NX, dtype=jnp.float32) / NX
    ramp = jnp.exp(jnp.log(3.0) * rows)[None, :, None]
    value = noise * ramp
    return jnp.clip(value, -30.0, 30.0)


def touch_ends(drawn, own_key, smallest, high):
    spot = [jax.random.randint(jax.random.fold_in(own_key, axis), (), 0, length) for axis, length in enumerate(drawn.shape)]
    longest = drawn.shape.index(max(drawn.shape))
    next_to = spot[:longest] + [(spot[longest] + 1) % drawn.shape[longest]] + spot[longest + 1:]
    return drawn.at[tuple(spot)].set(smallest).at[tuple(next_to)].set(high)


def shard_levels(key, dims, cuts, low, top_value):
    loudness = 1.0
    for dim, parts in cuts:
        heights = jax.random.uniform(jax.random.fold_in(jax.random.fold_in(key, 6), dim), (parts,), jnp.float32, low / len(cuts), top_value / len(cuts))
        loudness = loudness * jnp.repeat(jnp.exp(heights), dims[dim] // parts).reshape((-1,) + (1,) * (len(dims) - 1 - dim))
    return loudness


def setup_inputs(seed: int = 0) -> dict:
    streams_of = jax.random.split(jax.random.key(seed), 7)
    return {
        "right_side": draw_right_side(jax.random.fold_in(streams_of[6], 71), 0),
        "row_conduct": jnp.clip(jnp.exp(math.log(2.0) - 1.3862944 * jax.random.uniform(streams_of[1], (LAYERS, NX, NY), jnp.float32) ** shard_levels(streams_of[1], (LAYERS, NX, NY), ((0, 2), (1, 4), (2, 4)), -0.2, 0.2)), 0.5, 2.0),
        "column_conduct": jnp.clip(jnp.exp(math.log(2.0) - 1.3862944 * jax.random.uniform(streams_of[2], (LAYERS, NX, NY), jnp.float32) ** shard_levels(streams_of[2], (LAYERS, NX, NY), ((0, 2), (1, 4), (2, 4)), -0.2, 0.2)), 0.5, 2.0),
        "via_conduct": jnp.clip(jnp.exp(math.log(4.0) - 2.0794415 * jax.random.uniform(streams_of[3], (LAYERS, NX, NY), jnp.float32) ** shard_levels(streams_of[3], (LAYERS, NX, NY), ((0, 2), (1, 4), (2, 4)), -0.2, 0.2)), 0.5, 4.0),
        "via_mask": touch_ends((jax.random.randint(streams_of[4], (LAYERS, NX, NY), 0, 4) < 3).astype(jnp.int32), jax.random.fold_in(streams_of[4], 1), 0, 1),
        "ground_conduct": jnp.clip(jnp.exp(math.log(0.1) - 2.3025851 * jax.random.uniform(streams_of[5], (LAYERS, NX, NY), jnp.float32) ** shard_levels(streams_of[5], (LAYERS, NX, NY), ((0, 2), (1, 4), (2, 4)), -0.2, 0.2)), 0.01, 0.1),
    }


def factor_layers(diagonal, vertical, vertical_below, carried):
    gains = []
    inverses = []
    previous = carried
    for index in range(diagonal.shape[0]):
        inverse = 1.0 / (diagonal[index] - vertical_below[index] * previous)
        previous = vertical[index] * inverse
        gains.append(previous)
        inverses.append(inverse)
    return jnp.stack(gains), jnp.stack(inverses)


def forward_layers(residual, vertical_below, inverses, carried):
    values = []
    previous = carried
    for index in range(residual.shape[0]):
        previous = (residual[index] + vertical_below[index] * previous) * inverses[index]
        values.append(previous)
    return jnp.stack(values)


def back_layers(forward, gains, carried):
    count = forward.shape[0]
    values = [None] * count
    following = carried
    for index in range(count - 1, -1, -1):
        following = forward[index] + gains[index] * following
        values[index] = following
    return jnp.stack(values)


def operate(field, coeffs):
    diagonal, row_conduct, row_upper, column_conduct, column_left, vertical, vertical_below = coeffs
    padded = jnp.pad(field, 1)
    return (diagonal * field
            - row_conduct * padded[1:-1, 2:, 1:-1]
            - row_upper * padded[1:-1, :-2, 1:-1]
            - column_conduct * padded[1:-1, 1:-1, 2:]
            - column_left * padded[1:-1, 1:-1, :-2]
            - vertical * padded[2:, 1:-1, 1:-1]
            - vertical_below * padded[:-2, 1:-1, 1:-1])


def reference(right_side, row_conduct, column_conduct, via_conduct, via_mask, ground_conduct):
    level = jnp.arange(LAYERS, dtype=jnp.int32)
    keep = (level < LAYERS - 1).astype(right_side.dtype)[:, None, None]
    vertical = via_conduct * via_mask.astype(right_side.dtype) * keep
    row_upper = jnp.concatenate([jnp.zeros_like(row_conduct[:, :1, :]), row_conduct[:, :-1, :]], axis=1)
    column_left = jnp.concatenate([jnp.zeros_like(column_conduct[:, :, :1]), column_conduct[:, :, :-1]], axis=2)
    vertical_below = jnp.concatenate([jnp.zeros_like(vertical[:1]), vertical[:-1]], axis=0)
    diagonal = ground_conduct + row_conduct + row_upper + column_conduct + column_left + vertical + vertical_below
    coeffs = (diagonal, row_conduct, row_upper, column_conduct, column_left, vertical, vertical_below)
    plane = jnp.zeros_like(right_side[0])
    gains, inverses = factor_layers(diagonal, vertical, vertical_below, plane)

    def precondition(residual):
        forward = forward_layers(residual, vertical_below, inverses, plane)
        return back_layers(forward, gains, plane)

    solution_field = jnp.zeros_like(right_side)
    residual = right_side
    precond = precondition(residual)
    direction = precond
    rho = jnp.sum(residual * precond)
    for step in range(ITERS):
        image = operate(direction, coeffs)
        alpha = rho / jnp.sum(direction * image)
        solution_field = solution_field + alpha * direction
        residual = residual - alpha * image
        if step + 1 < ITERS:
            precond = precondition(residual)
            rho_next = jnp.sum(residual * precond)
            direction = precond + (rho_next / rho) * direction
            rho = rho_next
    return solution_field, residual
```

```python
import jax
import jax.numpy as jnp
from jax import lax
from jax.experimental import pallas as pl
from jax.experimental.pallas import tpu as pltpu
from jax.sharding import PartitionSpec as P

GROUPS = 4
SUB = 8
LANE = 128


def kernel(
    r_hbm, rc_hbm, cc_hbm, via_hbm, mask_hbm, gr_hbm,
    x_hbm, res_hbm,
    R, RC, CC, VI, MK, GR, RU, CL, C, INV, ZP, YP, W, V,
    PV, PM, SF1, SG, SF2, PF1, PG, PF2, E,
    stage_row, stage_col, row_send, row_recv, col_send, col_recv, HL0, HL, HR,
    sums_send, sums_py, sums_px, sums_layer,
    load_sem, stage_sem, plane_send_sem, plane_recv_sem, swap_send_sem, swap_recv_sem,
    row_send_sem, row_recv_sem, col_send_sem, col_recv_sem,
    py_send_sem, py_recv_sem, px_send_sem, px_recv_sem, la_send_sem, la_recv_sem, out_sem,
):
    depth, rows, cols = r_hbm.shape
    npx, npy = lax.axis_size("px"), lax.axis_size("py")
    core, px, py = lax.axis_index("layer"), lax.axis_index("px"), lax.axis_index("py")
    other = 1 - core
    size = rows // GROUPS
    chunks = size // SUB

    def remote(src, dst, send_sem, recv_sem, where):
        return pltpu.make_async_remote_copy(
            src_ref=src, dst_ref=dst, send_sem=send_sem, recv_sem=recv_sem,
            device_id=where, device_id_type=pl.DeviceIdType.MESH)

    stage = [
        pltpu.make_async_copy(rc_hbm.at[:, pl.ds(rows - SUB, SUB), :], stage_row, stage_sem.at[0]),
        pltpu.make_async_copy(cc_hbm.at[:, :, pl.ds(cols - LANE, LANE)], stage_col, stage_sem.at[1]),
    ]
    for copy in stage:
        copy.start()
    own_planes = [
        pltpu.make_async_copy(via_hbm.at[depth - 1], PV, plane_recv_sem.at[0]),
        pltpu.make_async_copy(mask_hbm.at[depth - 1], PM, plane_recv_sem.at[1]),
    ]

    @pl.when(core == 0)
    def _():
        for copy in own_planes:
            copy.start()

    loads = []
    for g in range(GROUPS):
        here = pl.ds(g * size, size)
        padded = pl.ds(SUB + g * size, size)
        pairs = ((rc_hbm, RC, padded), (cc_hbm, CC, here), (via_hbm, VI, here),
                 (mask_hbm, MK, here), (gr_hbm, GR, here), (r_hbm, R, here))
        group = [pltpu.make_async_copy(src.at[:, here, :], dst.at[:, at, :], load_sem.at[g, n])
                 for n, (src, dst, at) in enumerate(pairs)]
        for copy in group:
            copy.start()
        loads.append(group)

    barrier = pltpu.get_barrier_semaphore()
    for d in range(1, npy):
        pl.semaphore_signal(barrier, inc=1, device_id={"py": lax.rem(py + d, npy)},
                            device_id_type=pl.DeviceIdType.MESH)
    for d in range(1, npx):
        pl.semaphore_signal(barrier, inc=1, device_id={"px": lax.rem(px + d, npx)},
                            device_id_type=pl.DeviceIdType.MESH)
    pl.semaphore_signal(barrier, inc=1, device_id={"layer": other}, device_id_type=pl.DeviceIdType.MESH)

    @pl.when(px == 0)
    def _():
        for n in range(3):
            row_recv[n, 0] = jnp.zeros((depth, 1, cols), jnp.float32)

    @pl.when(px == npx - 1)
    def _():
        for n in range(3):
            row_recv[n, 1] = jnp.zeros((depth, 1, cols), jnp.float32)

    @pl.when(py == 0)
    def _():
        for n in range(3):
            col_recv[n, 0] = jnp.zeros((SUB, rows), jnp.float32)

    @pl.when(py == npy - 1)
    def _():
        for n in range(3):
            col_recv[n, 1] = jnp.zeros((SUB, rows), jnp.float32)

    pl.semaphore_wait(barrier, npy + npx - 1)

    planes = [
        remote(via_hbm.at[depth - 1], PV, plane_send_sem.at[0], plane_recv_sem.at[0], {"layer": other}),
        remote(mask_hbm.at[depth - 1], PM, plane_send_sem.at[1], plane_recv_sem.at[1], {"layer": other}),
    ]

    @pl.when(core == 0)
    def _():
        for copy in planes:
            copy.start()

    lane = lax.broadcasted_iota(jnp.int32, (SUB, LANE), 1)
    sub = lax.broadcasted_iota(jnp.int32, (SUB, cols), 0)
    lane_tall = lax.broadcasted_iota(jnp.int32, (rows, LANE), 1)

    def row_copy(n, side):
        to = px + 1 if side == 0 else px - 1
        return remote(row_send.at[n, side], row_recv.at[n, side], row_send_sem.at[n, side],
                      row_recv_sem.at[n, side], {"px": to})

    def col_copy(n, side):
        to = py + 1 if side == 0 else py - 1
        return remote(col_send.at[n, side], col_recv.at[n, side], col_send_sem.at[n, side],
                      col_recv_sem.at[n, side], {"py": to})

    def guarded(n, sides, what):
        for side in sides:
            row_out = px < npx - 1 if side == 0 else px > 0
            col_out = py < npy - 1 if side == 0 else py > 0
            row_in = px > 0 if side == 0 else px < npx - 1
            col_in = py > 0 if side == 0 else py < npy - 1
            if what == "start":
                pl.when(col_out)(lambda s=side: col_copy(n, s).start())
                pl.when(row_out)(lambda s=side: row_copy(n, s).start())
            elif what == "recv":
                pl.when(row_in)(lambda s=side: row_copy(n, s).wait_recv())
                pl.when(col_in)(lambda s=side: col_copy(n, s).wait_recv())
            else:
                pl.when(row_out)(lambda s=side: row_copy(n, s).wait_send())
                pl.when(col_out)(lambda s=side: col_copy(n, s).wait_send())

    def pack_columns(tile_of, at):
        packed = jnp.zeros((rows, LANE), jnp.float32)
        for l in range(depth):
            column = jnp.broadcast_to(tile_of(l)[:, at:at + 1], (rows, LANE))
            packed = jnp.where(lane_tall == l, column, packed)
        return jnp.transpose(packed)[:SUB, :]

    def unpack_columns(n, side, dst):
        tall = jnp.transpose(jnp.concatenate(
            [col_recv[n, side], jnp.zeros((LANE - SUB, rows), jnp.float32)], axis=0))
        for l in range(depth):
            dst[l] = jnp.broadcast_to(tall[:, l:l + 1], (rows, LANE))

    def take_rows(n, sides, dst):
        for side in sides:
            at = SUB - 1 if side == 0 else SUB + rows
            for l in range(depth):
                dst[l, pl.ds(at, 1), :] = row_recv[n, side, l]

    for copy in stage:
        copy.wait()
    for l in range(depth):
        row_send[0, 0, l] = stage_row[l, SUB - 1:SUB, :]
    col_send[0, 0] = pack_columns(lambda l: stage_col[l], LANE - 1)
    guarded(0, (0,), "start")

    def shift_left(value, halo):
        rolled = pltpu.roll(value, cols - 1, 1)
        last = jnp.where(lane == LANE - 1, halo, rolled[:, cols - LANE:])
        return jnp.concatenate([rolled[:, :cols - LANE], last], axis=1)

    def shift_right(value, halo):
        rolled = pltpu.roll(value, 1, 1)
        first = jnp.where(lane == 0, halo, rolled[:, :LANE])
        return jnp.concatenate([first, rolled[:, LANE:]], axis=1)

    def from_above(value, before):
        return jnp.where(sub == 0, pltpu.roll(before, 1, 0), pltpu.roll(value, 1, 0))

    def from_below(value, after):
        return jnp.where(sub == SUB - 1, pltpu.roll(after, SUB - 1, 0), pltpu.roll(value, SUB - 1, 0))

    def folded(value):
        total = value[:, :LANE]
        for n in range(1, cols // LANE):
            total = total + value[:, n * LANE:(n + 1) * LANE]
        return total

    order = [k + core * (depth - 1 - 2 * k) for k in range(depth)]
    via_at = [k + core * (depth - 2 - 2 * k) for k in range(depth - 1)]

    def span(i, pad=0):
        return pl.ds(pl.multiple_of(i * SUB + pad, SUB), SUB)

    def swap(n, src, dst, g):
        here = pl.ds(g * size, size)
        return remote(src.at[here, :], dst.at[here, :], swap_send_sem.at[n, g], swap_recv_sem.at[n, g],
                      {"layer": other})

    guarded(0, (0,), "recv")
    take_rows(0, (0,), RC)
    unpack_columns(0, 0, HL0)

    @pl.when(core == 0)
    def _():
        for copy in own_planes:
            copy.wait()

    @pl.when(core == 1)
    def _():
        for copy in planes:
            copy.wait_recv()

    def factor(i, carry):
        here = span(i)
        before_c = before_g = before_f = None
        for k in range(depth):
            l = order[k]
            rc = RC[l, span(i, SUB), :]
            ru = from_above(rc, RC[l, here, :])
            cc = CC[l, here, :]
            cl = shift_right(cc, HL0[l, here, :])
            RU[l, here, :] = ru
            CL[l, here, :] = cl
            if k < depth - 1:
                c = VI[via_at[k], here, :] * MK[via_at[k], here, :].astype(jnp.float32)
            else:
                c = PV[here, :] * PM[here, :].astype(jnp.float32)
            diagonal = GR[l, here, :] + rc + ru + cc + cl + c
            r = R[l, here, :]
            if k:
                diagonal = (diagonal + before_c) - before_c * before_g
                r = r + before_c * before_f
            inverse = 1.0 / diagonal
            f = r * inverse
            g = c * inverse
            C[k, here, :] = c
            INV[l, here, :] = inverse
            ZP[l, span(i, SUB), :] = f
            before_c, before_g, before_f = c, g, f
        SF1[here, :] = before_f
        SG[here, :] = before_g
        return carry

    for g in range(GROUPS):
        for copy in loads[g]:
            copy.wait()
        lax.fori_loop(g * chunks, (g + 1) * chunks, factor, 0)
        swap(0, SF1, PF1, g).start()
        swap(1, SG, PG, g).start()

    def back_first(i, total):
        here = span(i)
        own_g = SG[here, :]
        e = 1.0 / (1.0 - own_g * PG[here, :])
        E[here, :] = e
        value = (SF1[here, :] + own_g * PF1[here, :]) * e
        ZP[order[-1], span(i, SUB), :] = value
        total = total + folded(value * R[order[-1], here, :])
        for k in range(depth - 2, -1, -1):
            l = order[k]
            value = ZP[l, span(i, SUB), :] + C[k, here, :] * INV[l, here, :] * value
            ZP[l, span(i, SUB), :] = value
            total = total + folded(value * R[l, here, :])
        return total

    zero = jnp.zeros((SUB, LANE), jnp.float32)
    b0 = zero
    for g in range(GROUPS):
        swap(0, SF1, PF1, g).wait_recv()
        swap(1, SG, PG, g).wait_recv()
        b0 = lax.fori_loop(g * chunks, (g + 1) * chunks, back_first, b0)

    def send_halos(n, field):
        inner = pl.ds(SUB, rows)
        for l in range(depth):
            row_send[n, 0, l] = field[l, pl.ds(SUB + rows - 1, 1), :]
            row_send[n, 1, l] = field[l, pl.ds(SUB, 1), :]
        col_send[n, 0] = pack_columns(lambda l: field[l, inner, cols - LANE:], LANE - 1)
        col_send[n, 1] = pack_columns(lambda l: field[l, inner, :LANE], 0)
        guarded(n, (0, 1), "start")

    def recv_halos(n, field):
        guarded(n, (0, 1), "recv")
        take_rows(n, (0, 1), field)
        unpack_columns(n, 0, HL)
        unpack_columns(n, 1, HR)

    def lateral(field, l, i):
        here = span(i)
        value = field[l, span(i, SUB), :]
        total = RC[l, span(i, SUB), :] * from_below(value, field[l, span(i, 2 * SUB), :])
        total = total + RU[l, here, :] * from_above(value, field[l, here, :])
        total = total + CC[l, here, :] * shift_left(value, HR[l, here, :])
        total = total + CL[l, here, :] * shift_right(value, HL[l, here, :])
        return value, total

    send_halos(1, ZP)
    recv_halos(1, ZP)

    def image_first(i, total):
        here = span(i)
        before_f = None
        for k in range(depth):
            l = order[k]
            value, around = lateral(ZP, l, i)
            w = R[l, here, :] - around
            W[l, here, :] = w
            total = total + folded(value * w)
            if k:
                w = w + C[k - 1, here, :] * before_f
            before_f = w * INV[l, here, :]
            YP[l, span(i, SUB), :] = before_f
        SF2[here, :] = before_f
        return total

    g00 = zero
    for g in range(GROUPS):
        g00 = lax.fori_loop(g * chunks, (g + 1) * chunks, image_first, g00)
        swap(2, SF2, PF2, g).start()

    def back_second(i, total):
        here = span(i)
        value = (SF2[here, :] + SG[here, :] * PF2[here, :]) * E[here, :]
        YP[order[-1], span(i, SUB), :] = value
        total = total + folded(value * W[order[-1], here, :])
        for k in range(depth - 2, -1, -1):
            l = order[k]
            value = YP[l, span(i, SUB), :] + C[k, here, :] * INV[l, here, :] * value
            YP[l, span(i, SUB), :] = value
            total = total + folded(value * W[l, here, :])
        return total

    g01 = zero
    for g in range(GROUPS):
        swap(2, SF2, PF2, g).wait_recv()
        g01 = lax.fori_loop(g * chunks, (g + 1) * chunks, back_second, g01)

    send_halos(2, YP)
    recv_halos(2, YP)

    def image_second(i, total):
        here = span(i)
        for l in range(depth):
            value, around = lateral(YP, l, i)
            v = W[l, here, :] - around
            V[l, here, :] = v
            total = total + folded(value * v)
        return total

    g11 = lax.fori_loop(0, rows // SUB, image_second, zero)

    parts = [jnp.sum(value, axis=0, keepdims=True) for value in (b0, g00, g01, g11)]
    partial = jnp.concatenate(parts + [jnp.zeros((SUB - 4, LANE), jnp.float32)], axis=0)

    def all_sum(partial, stage_at, axis, me, count, buffer, send_sem, recv_sem):
        sums_send[stage_at] = partial
        buffer[me] = partial

        def copy(d, slot):
            return remote(sums_send.at[stage_at], buffer.at[slot], send_sem.at[d], recv_sem.at[slot],
                          {axis: lax.rem(me + d, count)})

        for d in range(1, count):
            copy(d, me).start()
        for d in range(1, count):
            copy(d, lax.rem(me + count - d, count)).wait_recv()
        for d in range(1, count):
            copy(d, me).wait_send()
        total = buffer[0]
        for n in range(1, count):
            total = total + buffer[n]
        return total

    partial = all_sum(partial, 0, "layer", core, 2, sums_layer, la_send_sem, la_recv_sem)
    partial = all_sum(partial, 1, "py", py, npy, sums_py, py_send_sem, py_recv_sem)
    partial = all_sum(partial, 2, "px", px, npx, sums_px, px_send_sem, px_recv_sem)
    flat = jnp.sum(partial, axis=1, keepdims=True)
    base = flat[1:2, :]
    h0 = flat[0:1, :] / base
    h1 = flat[2:3, :] / base
    h2 = flat[3:4, :] / base
    det = h2 - h1 * h1
    c0 = (h0 * h2 - h1) / det
    c1 = (1.0 - h1 * h0) / det

    def finish(i, carry):
        here = span(i)
        for l in range(depth):
            inner = span(i, SUB)
            YP[l, inner, :] = c0 * ZP[l, inner, :] + c1 * YP[l, inner, :]
            V[l, here, :] = R[l, here, :] - c0 * W[l, here, :] - c1 * V[l, here, :]
        return carry

    outs = []
    for g in range(GROUPS):
        lax.fori_loop(g * chunks, (g + 1) * chunks, finish, 0)
        here = pl.ds(g * size, size)
        pair = [
            pltpu.make_async_copy(YP.at[:, pl.ds(SUB + g * size, size), :], x_hbm.at[:, here, :], out_sem.at[g, 0]),
            pltpu.make_async_copy(V.at[:, here, :], res_hbm.at[:, here, :], out_sem.at[g, 1]),
        ]
        for copy in pair:
            copy.start()
        outs += pair

    @pl.when(core == 0)
    def _():
        for copy in planes:
            copy.wait_send()

    guarded(0, (0,), "send")
    guarded(1, (0, 1), "send")
    guarded(2, (0, 1), "send")
    for g in range(GROUPS):
        swap(0, SF1, PF1, g).wait_send()
        swap(1, SG, PG, g).wait_send()
        swap(2, SF2, PF2, g).wait_send()
    for copy in outs:
        copy.wait()


def shards(right_side, row_conduct, column_conduct, via_conduct, via_mask, ground_conduct):
    depth, rows, cols = right_side.shape
    npx, npy = lax.axis_size("px"), lax.axis_size("py")
    f32 = jnp.float32
    block = pltpu.VMEM((depth, rows, cols), f32)
    plane = pltpu.VMEM((rows, cols), f32)
    dma = pltpu.SemaphoreType.DMA
    scratch = [
        block, pltpu.VMEM((depth, rows + SUB, cols), f32), block, block,
        pltpu.VMEM((depth, rows, cols), jnp.int32), block, block, block, block, block,
        pltpu.VMEM((depth, rows + 2 * SUB, cols), f32), pltpu.VMEM((depth, rows + 2 * SUB, cols), f32),
        block, block,
        plane, pltpu.VMEM((rows, cols), jnp.int32), plane, plane, plane, plane, plane, plane, plane,
        pltpu.VMEM((depth, SUB, cols), f32), pltpu.VMEM((depth, rows, LANE), f32),
        pltpu.VMEM((3, 2, depth, 1, cols), f32), pltpu.VMEM((3, 2, depth, 1, cols), f32),
        pltpu.VMEM((3, 2, SUB, rows), f32), pltpu.VMEM((3, 2, SUB, rows), f32),
        pltpu.VMEM((depth, rows, LANE), f32), pltpu.VMEM((depth, rows, LANE), f32),
        pltpu.VMEM((depth, rows, LANE), f32),
        pltpu.VMEM((3, SUB, LANE), f32), pltpu.VMEM((npy, SUB, LANE), f32),
        pltpu.VMEM((npx, SUB, LANE), f32), pltpu.VMEM((2, SUB, LANE), f32),
        dma((GROUPS, 6)), dma((2,)), dma((2,)), dma((2,)), dma((3, GROUPS)), dma((3, GROUPS)),
        dma((3, 2)), dma((3, 2)), dma((3, 2)), dma((3, 2)),
        dma((npy,)), dma((npy,)), dma((npx,)), dma((npx,)), dma((2,)), dma((2,)), dma((GROUPS, 2)),
    ]
    anywhere = pl.BlockSpec(memory_space=pl.ANY)
    out = jax.ShapeDtypeStruct((depth, rows, cols), f32)
    return pl.pallas_call(
        kernel,
        out_shape=(out, out),
        in_specs=[anywhere] * 6,
        out_specs=(anywhere, anywhere),
        scratch_shapes=scratch,
        compiler_params=pltpu.CompilerParams(
            collective_id=0, has_side_effects=True, vmem_limit_bytes=60 * 1024 * 1024),
        name="pcg",
    )(right_side, row_conduct, column_conduct, via_conduct, via_mask, ground_conduct)


def solution(mesh):
    spec = P("layer", "px", "py")
    return jax.shard_map(shards, mesh=mesh, in_specs=(spec,) * 6, out_specs=(spec, spec), check_vma=False)
```

```python
import jax
import jax.numpy as jnp
from jax import lax
from jax.experimental import pallas as pl
from jax.experimental.pallas import tpu as pltpu
from jax.sharding import PartitionSpec as P

GROUPS = 4
SUB = 8
LANE = 128
VMEM_LIMIT = 52 * 1024 * 1024


def kernel(
    r_hbm, rc_hbm, cc_hbm, via_hbm, mask_hbm, gr_hbm,
    ZP, YP, W, V, R, coef_z, coef_y, coef_w, coef_v,
    RC, CC, VI, MK, GR, RU, CL, C, INV,
    PV, PM, SF1, SG, SF2, PF1, PG, PF2, E,
    stage_row, stage_col, row_send, row_recv, col_send, col_recv, HL0, HL, HR,
    sums_send, sums_plane, sums_px,
    load_sem, stage_sem, plane_send_sem, plane_recv_sem, swap_send_sem, swap_recv_sem,
    row_send_sem, row_recv_sem, col_send_sem, col_recv_sem,
    plane_sum_send, plane_sum_recv, px_send_sem, px_recv_sem,
):
    depth, rows, cols = r_hbm.shape
    npx, npy = lax.axis_size("px"), lax.axis_size("py")
    core, px, py = lax.axis_index("layer"), lax.axis_index("px"), lax.axis_index("py")
    other = 1 - core
    size = rows // GROUPS
    chunks = size // SUB

    def remote(src, dst, send_sem, recv_sem, where):
        return pltpu.make_async_remote_copy(
            src_ref=src, dst_ref=dst, send_sem=send_sem, recv_sem=recv_sem,
            device_id=where, device_id_type=pl.DeviceIdType.MESH)

    stage = [
        pltpu.make_async_copy(rc_hbm.at[:, pl.ds(rows - SUB, SUB), :], stage_row, stage_sem.at[0]),
        pltpu.make_async_copy(cc_hbm.at[:, :, pl.ds(cols - LANE, LANE)], stage_col, stage_sem.at[1]),
    ]
    for copy in stage:
        copy.start()
    own_planes = [
        pltpu.make_async_copy(via_hbm.at[depth - 1], PV, plane_recv_sem.at[0]),
        pltpu.make_async_copy(mask_hbm.at[depth - 1], PM, plane_recv_sem.at[1]),
    ]

    @pl.when(core == 0)
    def _():
        for copy in own_planes:
            copy.start()

    loads = []
    for g in range(GROUPS):
        here = pl.ds(g * size, size)
        padded = pl.ds(SUB + g * size, size)
        pairs = ((rc_hbm, RC, padded), (cc_hbm, CC, here), (via_hbm, VI, here),
                 (mask_hbm, MK, here), (gr_hbm, GR, here), (r_hbm, R, here))
        group = [pltpu.make_async_copy(src.at[:, here, :], dst.at[:, at, :], load_sem.at[g, n])
                 for n, (src, dst, at) in enumerate(pairs)]
        for copy in group:
            copy.start()
        loads.append(group)

    barrier = pltpu.get_barrier_semaphore()
    wide = 2 * npy
    mine = core * npy + py

    def in_plane(d):
        at = lax.rem(mine + d, wide)
        return {"layer": at // npy, "py": lax.rem(at, npy)}

    def in_px(d):
        return {"px": lax.rem(px + d, npx)}

    for peers, count in ((in_plane, wide), (in_px, npx)):
        for d in range(1, count):
            pl.semaphore_signal(barrier, inc=1, device_id=peers(d), device_id_type=pl.DeviceIdType.MESH)

    @pl.when(px == 0)
    def _():
        for n in range(3):
            row_recv[n, 0] = jnp.zeros((depth, 1, cols), jnp.float32)

    @pl.when(px == npx - 1)
    def _():
        for n in range(3):
            row_recv[n, 1] = jnp.zeros((depth, 1, cols), jnp.float32)

    @pl.when(py == 0)
    def _():
        for n in range(3):
            col_recv[n, 0] = jnp.zeros((SUB, rows), jnp.float32)

    @pl.when(py == npy - 1)
    def _():
        for n in range(3):
            col_recv[n, 1] = jnp.zeros((SUB, rows), jnp.float32)

    pl.semaphore_wait(barrier, wide + npx - 2)

    planes = [
        remote(via_hbm.at[depth - 1], PV, plane_send_sem.at[0], plane_recv_sem.at[0], {"layer": other}),
        remote(mask_hbm.at[depth - 1], PM, plane_send_sem.at[1], plane_recv_sem.at[1], {"layer": other}),
    ]

    @pl.when(core == 0)
    def _():
        for copy in planes:
            copy.start()

    lane = lax.broadcasted_iota(jnp.int32, (SUB, LANE), 1)
    sub = lax.broadcasted_iota(jnp.int32, (SUB, cols), 0)
    lane_tall = lax.broadcasted_iota(jnp.int32, (rows, LANE), 1)

    def row_copy(n, side):
        to = px + 1 if side == 0 else px - 1
        return remote(row_send.at[n, side], row_recv.at[n, side], row_send_sem.at[n, side],
                      row_recv_sem.at[n, side], {"px": to})

    def col_copy(n, side):
        to = py + 1 if side == 0 else py - 1
        return remote(col_send.at[n, side], col_recv.at[n, side], col_send_sem.at[n, side],
                      col_recv_sem.at[n, side], {"py": to})

    def guarded(n, sides, what):
        for side in sides:
            row_out = px < npx - 1 if side == 0 else px > 0
            col_out = py < npy - 1 if side == 0 else py > 0
            row_in = px > 0 if side == 0 else px < npx - 1
            col_in = py > 0 if side == 0 else py < npy - 1
            if what == "start":
                pl.when(col_out)(lambda s=side: col_copy(n, s).start())
                pl.when(row_out)(lambda s=side: row_copy(n, s).start())
            elif what == "recv":
                pl.when(row_in)(lambda s=side: row_copy(n, s).wait_recv())
                pl.when(col_in)(lambda s=side: col_copy(n, s).wait_recv())
            else:
                pl.when(row_out)(lambda s=side: row_copy(n, s).wait_send())
                pl.when(col_out)(lambda s=side: col_copy(n, s).wait_send())

    def pack_columns(tile_of, at):
        packed = jnp.zeros((rows, LANE), jnp.float32)
        for l in range(depth):
            column = jnp.broadcast_to(tile_of(l)[:, at:at + 1], (rows, LANE))
            packed = jnp.where(lane_tall == l, column, packed)
        return jnp.transpose(packed)[:SUB, :]

    def unpack_columns(n, side, dst):
        tall = jnp.transpose(jnp.concatenate(
            [col_recv[n, side], jnp.zeros((LANE - SUB, rows), jnp.float32)], axis=0))
        for l in range(depth):
            dst[l] = jnp.broadcast_to(tall[:, l:l + 1], (rows, LANE))

    def take_rows(n, sides, dst):
        for side in sides:
            at = SUB - 1 if side == 0 else SUB + rows
            for l in range(depth):
                dst[l, pl.ds(at, 1), :] = row_recv[n, side, l]

    for copy in stage:
        copy.wait()
    for l in range(depth):
        row_send[0, 0, l] = stage_row[l, SUB - 1:SUB, :]
    col_send[0, 0] = pack_columns(lambda l: stage_col[l], LANE - 1)
    guarded(0, (0,), "start")

    def shift_left(value, halo):
        rolled = pltpu.roll(value, cols - 1, 1)
        last = jnp.where(lane == LANE - 1, halo, rolled[:, cols - LANE:])
        return jnp.concatenate([rolled[:, :cols - LANE], last], axis=1)

    def shift_right(value, halo):
        rolled = pltpu.roll(value, 1, 1)
        first = jnp.where(lane == 0, halo, rolled[:, :LANE])
        return jnp.concatenate([first, rolled[:, LANE:]], axis=1)

    def from_above(value, before):
        return jnp.where(sub == 0, pltpu.roll(before, 1, 0), pltpu.roll(value, 1, 0))

    def from_below(value, after):
        return jnp.where(sub == SUB - 1, pltpu.roll(after, SUB - 1, 0), pltpu.roll(value, SUB - 1, 0))

    def folded(value):
        total = value[:, :LANE]
        for n in range(1, cols // LANE):
            total = total + value[:, n * LANE:(n + 1) * LANE]
        return total

    order = [k + core * (depth - 1 - 2 * k) for k in range(depth)]
    via_at = [k + core * (depth - 2 - 2 * k) for k in range(depth - 1)]

    def span(i, pad=0):
        return pl.ds(pl.multiple_of(i * SUB + pad, SUB), SUB)

    def swap(n, src, dst, g):
        here = pl.ds(g * size, size)
        return remote(src.at[here, :], dst.at[here, :], swap_send_sem.at[n, g], swap_recv_sem.at[n, g],
                      {"layer": other})

    guarded(0, (0,), "recv")
    take_rows(0, (0,), RC)
    unpack_columns(0, 0, HL0)

    @pl.when(core == 0)
    def _():
        for copy in own_planes:
            copy.wait()

    @pl.when(core == 1)
    def _():
        for copy in planes:
            copy.wait_recv()

    def factor(i, carry):
        here = span(i)
        before_c = before_g = before_f = None
        for k in range(depth):
            l = order[k]
            rc = RC[l, span(i, SUB), :]
            ru = from_above(rc, RC[l, here, :])
            cc = CC[l, here, :]
            cl = shift_right(cc, HL0[l, here, :])
            RU[l, here, :] = ru
            CL[l, here, :] = cl
            if k < depth - 1:
                c = VI[via_at[k], here, :] * MK[via_at[k], here, :].astype(jnp.float32)
            else:
                c = PV[here, :] * PM[here, :].astype(jnp.float32)
            diagonal = GR[l, here, :] + rc + ru + cc + cl + c
            r = R[l, here, :]
            if k:
                diagonal = (diagonal + before_c) - before_c * before_g
                r = r + before_c * before_f
            inverse = 1.0 / diagonal
            f = r * inverse
            g = c * inverse
            C[k, here, :] = c
            INV[l, here, :] = inverse
            ZP[l, span(i, SUB), :] = f
            before_c, before_g, before_f = c, g, f
        SF1[here, :] = before_f
        SG[here, :] = before_g
        return carry

    for g in range(GROUPS):
        for copy in loads[g]:
            copy.wait()
        lax.fori_loop(g * chunks, (g + 1) * chunks, factor, 0)
        swap(0, SF1, PF1, g).start()
        swap(1, SG, PG, g).start()

    def back_first(i, total):
        here = span(i)
        own_g = SG[here, :]
        e = 1.0 / (1.0 - own_g * PG[here, :])
        E[here, :] = e
        value = (SF1[here, :] + own_g * PF1[here, :]) * e
        ZP[order[-1], span(i, SUB), :] = value
        total = total + folded(value * R[order[-1], here, :])
        for k in range(depth - 2, -1, -1):
            l = order[k]
            value = ZP[l, span(i, SUB), :] + C[k, here, :] * INV[l, here, :] * value
            ZP[l, span(i, SUB), :] = value
            total = total + folded(value * R[l, here, :])
        return total

    zero = jnp.zeros((SUB, LANE), jnp.float32)
    b0 = zero
    for g in range(GROUPS):
        swap(0, SF1, PF1, g).wait_recv()
        swap(1, SG, PG, g).wait_recv()
        b0 = lax.fori_loop(g * chunks, (g + 1) * chunks, back_first, b0)

    def send_halos(n, field):
        inner = pl.ds(SUB, rows)
        for l in range(depth):
            row_send[n, 0, l] = field[l, pl.ds(SUB + rows - 1, 1), :]
            row_send[n, 1, l] = field[l, pl.ds(SUB, 1), :]
        col_send[n, 0] = pack_columns(lambda l: field[l, inner, cols - LANE:], LANE - 1)
        col_send[n, 1] = pack_columns(lambda l: field[l, inner, :LANE], 0)
        guarded(n, (0, 1), "start")

    def recv_halos(n, field):
        guarded(n, (0, 1), "recv")
        take_rows(n, (0, 1), field)
        unpack_columns(n, 0, HL)
        unpack_columns(n, 1, HR)

    def lateral(field, l, i):
        here = span(i)
        value = field[l, span(i, SUB), :]
        total = RC[l, span(i, SUB), :] * from_below(value, field[l, span(i, 2 * SUB), :])
        total = total + RU[l, here, :] * from_above(value, field[l, here, :])
        total = total + CC[l, here, :] * shift_left(value, HR[l, here, :])
        total = total + CL[l, here, :] * shift_right(value, HL[l, here, :])
        return value, total

    send_halos(1, ZP)
    recv_halos(1, ZP)

    def image_first(i, total):
        here = span(i)
        before_f = None
        for k in range(depth):
            l = order[k]
            value, around = lateral(ZP, l, i)
            w = R[l, here, :] - around
            W[l, here, :] = w
            total = (total[0] + folded(value * w), total[1] + folded(value * around))
            if k:
                w = w + C[k - 1, here, :] * before_f
            before_f = w * INV[l, here, :]
            YP[l, span(i, SUB), :] = before_f
        SF2[here, :] = before_f
        return total

    g00 = (zero, zero)
    for g in range(GROUPS):
        g00 = lax.fori_loop(g * chunks, (g + 1) * chunks, image_first, g00)
        swap(2, SF2, PF2, g).start()
    g00, s1 = g00

    def back_second(i, total):
        here = span(i)
        value = (SF2[here, :] + SG[here, :] * PF2[here, :]) * E[here, :]
        YP[order[-1], span(i, SUB), :] = value
        total = total + folded(value * W[order[-1], here, :])
        for k in range(depth - 2, -1, -1):
            l = order[k]
            value = YP[l, span(i, SUB), :] + C[k, here, :] * INV[l, here, :] * value
            YP[l, span(i, SUB), :] = value
            total = total + folded(value * W[l, here, :])
        return total

    g01 = zero
    for g in range(GROUPS):
        swap(2, SF2, PF2, g).wait_recv()
        g01 = lax.fori_loop(g * chunks, (g + 1) * chunks, back_second, g01)

    send_halos(2, YP)
    recv_halos(2, YP)

    def image_second(i, total):
        here = span(i)
        for l in range(depth):
            value, around = lateral(YP, l, i)
            V[l, here, :] = around
            z = ZP[l, span(i, SUB), :]
            total = (total[0] + folded(value * (W[l, here, :] - around)),
                     total[1] + folded(z * around), total[2] + folded((z - value) * around))
        return total

    g11, q01, q11 = lax.fori_loop(0, rows // SUB, image_second, (zero, zero, zero))

    parts = [jnp.sum(value, axis=0, keepdims=True) for value in (b0, g00, g01, g11, s1, q01, q11)]
    partial = jnp.concatenate(parts + [jnp.zeros((1, LANE), jnp.float32)], axis=0)

    def all_sum(partial, stage_at, peers, me, count, buffer, send_sem, recv_sem):
        sums_send[stage_at] = partial
        buffer[me] = partial

        def copy(d, slot):
            return remote(sums_send.at[stage_at], buffer.at[slot], send_sem.at[d], recv_sem.at[slot], peers(d))

        for d in range(1, count):
            copy(d, me).start()
        for d in range(1, count):
            copy(d, lax.rem(me + count - d, count)).wait_recv()
        for d in range(1, count):
            copy(d, me).wait_send()
        total = buffer[0]
        for n in range(1, count):
            total = total + buffer[n]
        return total

    partial = all_sum(partial, 0, in_plane, mine, wide, sums_plane, plane_sum_send, plane_sum_recv)
    partial = all_sum(partial, 1, in_px, px, npx, sums_px, px_send_sem, px_recv_sem)
    flat = jnp.broadcast_to(jnp.sum(partial, axis=1, keepdims=True), (SUB, LANE))
    b0, g00, g01, g11, s1, q01, q11 = (flat[n:n + 1, :] / flat[1:2, :] for n in range(7))
    det_q = q11 - q01 * q01
    a_q = (b0 * q11 - q01 * s1) / det_q
    b_q = (s1 - q01 * b0) / det_q
    det_y = g11 - g01 * g01
    c1 = (1.0 - g01 * b0) / det_y
    c0 = (b0 * g11 - g01) / det_y
    take_q = q01 * q01 * g11 <= g01 * g01 * q11
    a = jnp.where(take_q, a_q, c0 + c1)
    b = jnp.where(take_q, b_q, -c1)

    def spread(value):
        return jnp.concatenate([value] * (cols // LANE), axis=1)

    coef_z[...] = spread(a + b)
    coef_y[...] = spread(-b)
    coef_w[...] = spread(a)
    coef_v[...] = spread(b)

    @pl.when(core == 0)
    def _():
        for copy in planes:
            copy.wait_send()

    guarded(0, (0,), "send")
    guarded(1, (0, 1), "send")
    guarded(2, (0, 1), "send")
    for g in range(GROUPS):
        swap(0, SF1, PF1, g).wait_send()
        swap(1, SG, PG, g).wait_send()
        swap(2, SF2, PF2, g).wait_send()


def shards(right_side, row_conduct, column_conduct, via_conduct, via_mask, ground_conduct):
    depth, rows, cols = right_side.shape
    npx, npy = lax.axis_size("px"), lax.axis_size("py")
    f32 = jnp.float32
    block = pltpu.VMEM((depth, rows, cols), f32)
    plane = pltpu.VMEM((rows, cols), f32)
    dma = pltpu.SemaphoreType.DMA
    scratch = [
        pltpu.VMEM((depth, rows + SUB, cols), f32), block, block,
        pltpu.VMEM((depth, rows, cols), jnp.int32), block, block, block, block, block,
        plane, pltpu.VMEM((rows, cols), jnp.int32), plane, plane, plane, plane, plane, plane, plane,
        pltpu.VMEM((depth, SUB, cols), f32), pltpu.VMEM((depth, rows, LANE), f32),
        pltpu.VMEM((3, 2, depth, 1, cols), f32), pltpu.VMEM((3, 2, depth, 1, cols), f32),
        pltpu.VMEM((3, 2, SUB, rows), f32), pltpu.VMEM((3, 2, SUB, rows), f32),
        pltpu.VMEM((depth, rows, LANE), f32), pltpu.VMEM((depth, rows, LANE), f32),
        pltpu.VMEM((depth, rows, LANE), f32),
        pltpu.VMEM((2, SUB, LANE), f32), pltpu.VMEM((2 * npy, SUB, LANE), f32),
        pltpu.VMEM((npx, SUB, LANE), f32),
        dma((GROUPS, 6)), dma((2,)), dma((2,)), dma((2,)), dma((3, GROUPS)), dma((3, GROUPS)),
        dma((3, 2)), dma((3, 2)), dma((3, 2)), dma((3, 2)),
        dma((2 * npy,)), dma((2 * npy,)), dma((npx,)), dma((npx,)),
    ]
    anywhere = pl.BlockSpec(memory_space=pl.ANY)
    padded = pltpu.VMEM((depth, rows + 2 * SUB, cols), f32)
    near = pl.BlockSpec(memory_space=pltpu.VMEM)
    row = pltpu.VMEM((1, cols), f32)
    z, y, w, v, r, coef_z, coef_y, coef_w, coef_v = pl.pallas_call(
        kernel,
        out_shape=(padded, padded, block, block, block, row, row, row, row),
        in_specs=[anywhere] * 6,
        out_specs=(near,) * 9,
        scratch_shapes=scratch,
        compiler_params=pltpu.CompilerParams(
            collective_id=0, has_side_effects=True, vmem_limit_bytes=VMEM_LIMIT),
        name="pcg",
    )(right_side, row_conduct, column_conduct, via_conduct, via_mask, ground_conduct)
    inner = slice(SUB, SUB + rows)
    return coef_z * z[:, inner, :] + coef_y * y[:, inner, :], r - coef_w * w - coef_v * v


def solution(mesh):
    spec = P("layer", "px", "py")
    return jax.shard_map(shards, mesh=mesh, in_specs=(spec,) * 6, out_specs=(spec, spec), check_vma=False)
```

```python
import jax
import jax.numpy as jnp
from jax import lax
from jax.experimental import pallas as pl
from jax.experimental.pallas import tpu as pltpu
from jax.sharding import PartitionSpec as P

GROUPS = 4
SUB = 8
LANE = 128
VMEM_LIMIT = 52 * 1024 * 1024


def kernel(
    r_hbm, rc_hbm, cc_hbm, via_hbm, mask_hbm, gr_hbm,
    ZP, YP, W, V, R, coef_z, coef_y, coef_w, coef_v,
    RC, CC, VI, MK, GR, RU, CL, C, INV,
    PV, PM, SF1, SG, SF2, PF1, PG, PF2, E,
    stage_row, stage_col, row_send, row_recv, col_send, col_recv, HL0,
    sums_send, sums_plane, sums_px,
    load_sem, stage_sem, plane_send_sem, plane_recv_sem, swap_send_sem, swap_recv_sem,
    row_send_sem, row_recv_sem, col_send_sem, col_recv_sem,
    plane_sum_send, plane_sum_recv, px_send_sem, px_recv_sem,
):
    depth, rows, cols = r_hbm.shape
    npx, npy = lax.axis_size("px"), lax.axis_size("py")
    core, px, py = lax.axis_index("layer"), lax.axis_index("px"), lax.axis_index("py")
    other = 1 - core
    size = rows // GROUPS
    chunks = size // SUB

    def remote(src, dst, send_sem, recv_sem, where):
        return pltpu.make_async_remote_copy(
            src_ref=src, dst_ref=dst, send_sem=send_sem, recv_sem=recv_sem,
            device_id=where, device_id_type=pl.DeviceIdType.MESH)

    stage = [
        pltpu.make_async_copy(rc_hbm.at[:, pl.ds(rows - SUB, SUB), :], stage_row, stage_sem.at[0]),
        pltpu.make_async_copy(cc_hbm.at[:, :, pl.ds(cols - LANE, LANE)], stage_col, stage_sem.at[1]),
    ]
    for copy in stage:
        copy.start()
    own_planes = [
        pltpu.make_async_copy(via_hbm.at[depth - 1], PV, plane_recv_sem.at[0]),
        pltpu.make_async_copy(mask_hbm.at[depth - 1], PM, plane_recv_sem.at[1]),
    ]

    @pl.when(core == 0)
    def _():
        for copy in own_planes:
            copy.start()

    loads = []
    for g in range(GROUPS):
        here = pl.ds(g * size, size)
        padded = pl.ds(SUB + g * size, size)
        pairs = ((rc_hbm, RC, padded), (cc_hbm, CC, here), (via_hbm, VI, here),
                 (mask_hbm, MK, here), (gr_hbm, GR, here), (r_hbm, R, here))
        group = [pltpu.make_async_copy(src.at[:, here, :], dst.at[:, at, :], load_sem.at[g, n])
                 for n, (src, dst, at) in enumerate(pairs)]
        for copy in group:
            copy.start()
        loads.append(group)

    barrier = pltpu.get_barrier_semaphore()
    wide = 2 * npy
    mine = core * npy + py

    def in_plane(d):
        at = lax.rem(mine + d, wide)
        return {"layer": at // npy, "py": lax.rem(at, npy)}

    def in_px(d):
        return {"px": lax.rem(px + d, npx)}

    for peers, count in ((in_plane, wide), (in_px, npx)):
        for d in range(1, count):
            pl.semaphore_signal(barrier, inc=1, device_id=peers(d), device_id_type=pl.DeviceIdType.MESH)

    for field in (ZP, YP):
        field[:, pl.ds(0, SUB), :] = jnp.zeros((depth, SUB, cols), jnp.float32)
        field[:, pl.ds(SUB + rows, SUB), :] = jnp.zeros((depth, SUB, cols), jnp.float32)

    @pl.when(px == 0)
    def _():
        for n in range(3):
            row_recv[n, 0] = jnp.zeros((depth, 1, cols), jnp.float32)

    @pl.when(px == npx - 1)
    def _():
        for n in range(3):
            row_recv[n, 1] = jnp.zeros((depth, 1, cols), jnp.float32)

    @pl.when(py == 0)
    def _():
        for n in range(3):
            col_recv[n, 0] = jnp.zeros((SUB, rows), jnp.float32)

    @pl.when(py == npy - 1)
    def _():
        for n in range(3):
            col_recv[n, 1] = jnp.zeros((SUB, rows), jnp.float32)

    pl.semaphore_wait(barrier, wide + npx - 2)

    planes = [
        remote(via_hbm.at[depth - 1], PV, plane_send_sem.at[0], plane_recv_sem.at[0], {"layer": other}),
        remote(mask_hbm.at[depth - 1], PM, plane_send_sem.at[1], plane_recv_sem.at[1], {"layer": other}),
    ]

    @pl.when(core == 0)
    def _():
        for copy in planes:
            copy.start()

    lane = lax.broadcasted_iota(jnp.int32, (SUB, LANE), 1)
    sub = lax.broadcasted_iota(jnp.int32, (SUB, cols), 0)
    lane_tall = lax.broadcasted_iota(jnp.int32, (rows, LANE), 1)

    def row_copy(n, side):
        to = px + 1 if side == 0 else px - 1
        return remote(row_send.at[n, side], row_recv.at[n, side], row_send_sem.at[n, side],
                      row_recv_sem.at[n, side], {"px": to})

    def col_copy(n, side):
        to = py + 1 if side == 0 else py - 1
        return remote(col_send.at[n, side], col_recv.at[n, side], col_send_sem.at[n, side],
                      col_recv_sem.at[n, side], {"py": to})

    def guarded(n, sides, what):
        for side in sides:
            row_out = px < npx - 1 if side == 0 else px > 0
            col_out = py < npy - 1 if side == 0 else py > 0
            row_in = px > 0 if side == 0 else px < npx - 1
            col_in = py > 0 if side == 0 else py < npy - 1
            if what == "start":
                pl.when(col_out)(lambda s=side: col_copy(n, s).start())
                pl.when(row_out)(lambda s=side: row_copy(n, s).start())
            elif what == "recv":
                pl.when(row_in)(lambda s=side: row_copy(n, s).wait_recv())
                pl.when(col_in)(lambda s=side: col_copy(n, s).wait_recv())
            else:
                pl.when(row_out)(lambda s=side: row_copy(n, s).wait_send())
                pl.when(col_out)(lambda s=side: col_copy(n, s).wait_send())

    def pack_columns(tile_of, at):
        packed = jnp.zeros((rows, LANE), jnp.float32)
        for l in range(depth):
            column = jnp.broadcast_to(tile_of(l)[:, at:at + 1], (rows, LANE))
            packed = jnp.where(lane_tall == l, column, packed)
        return jnp.transpose(packed)[:SUB, :]

    def unpacked(n, side):
        return jnp.transpose(jnp.concatenate(
            [col_recv[n, side], jnp.zeros((LANE - SUB, rows), jnp.float32)], axis=0))

    for copy in stage:
        copy.wait()
    for l in range(depth):
        row_send[0, 0, l] = stage_row[l, SUB - 1:SUB, :]
    col_send[0, 0] = pack_columns(lambda l: stage_col[l], LANE - 1)
    guarded(0, (0,), "start")

    def shift_left(value, halo):
        rolled = pltpu.roll(value, cols - 1, 1)
        last = jnp.where(lane == LANE - 1, halo, rolled[:, cols - LANE:])
        return jnp.concatenate([rolled[:, :cols - LANE], last], axis=1)

    def shift_right(value, halo):
        rolled = pltpu.roll(value, 1, 1)
        first = jnp.where(lane == 0, halo, rolled[:, :LANE])
        return jnp.concatenate([first, rolled[:, LANE:]], axis=1)

    def from_above(value, before):
        return jnp.where(sub == 0, pltpu.roll(before, 1, 0), pltpu.roll(value, 1, 0))

    def from_below(value, after):
        return jnp.where(sub == SUB - 1, pltpu.roll(after, SUB - 1, 0), pltpu.roll(value, SUB - 1, 0))

    def folded(value):
        total = value[:, :LANE]
        for n in range(1, cols // LANE):
            total = total + value[:, n * LANE:(n + 1) * LANE]
        return total

    order = [k + core * (depth - 1 - 2 * k) for k in range(depth)]
    via_at = [k + core * (depth - 2 - 2 * k) for k in range(depth - 1)]

    def span(i, pad=0):
        return pl.ds(pl.multiple_of(i * SUB + pad, SUB), SUB)

    def swap(n, src, dst, g):
        here = pl.ds(g * size, size)
        return remote(src.at[here, :], dst.at[here, :], swap_send_sem.at[n, g], swap_recv_sem.at[n, g],
                      {"layer": other})

    guarded(0, (0,), "recv")
    tall = unpacked(0, 0)
    for l in range(depth):
        RC[l, pl.ds(SUB - 1, 1), :] = row_recv[0, 0, l]
        HL0[l] = jnp.broadcast_to(tall[:, l:l + 1], (rows, LANE))

    @pl.when(core == 0)
    def _():
        for copy in own_planes:
            copy.wait()

    @pl.when(core == 1)
    def _():
        for copy in planes:
            copy.wait_recv()

    def factor(i, carry):
        here = span(i)
        before_c = before_g = before_f = None
        for k in range(depth):
            l = order[k]
            rc = RC[l, span(i, SUB), :]
            ru = from_above(rc, RC[l, here, :])
            cc = CC[l, here, :]
            cl = shift_right(cc, HL0[l, here, :])
            RU[l, here, :] = ru
            CL[l, here, :] = cl
            if k < depth - 1:
                c = VI[via_at[k], here, :] * MK[via_at[k], here, :].astype(jnp.float32)
            else:
                c = PV[here, :] * PM[here, :].astype(jnp.float32)
            diagonal = GR[l, here, :] + rc + ru + cc + cl + c
            r = R[l, here, :]
            if k:
                diagonal = (diagonal + before_c) - before_c * before_g
                r = r + before_c * before_f
            inverse = 1.0 / diagonal
            f = r * inverse
            g = c * inverse
            C[k, here, :] = c
            INV[l, here, :] = inverse
            ZP[l, span(i, SUB), :] = f
            before_c, before_g, before_f = c, g, f
        SF1[here, :] = before_f
        SG[here, :] = before_g
        return carry

    for g in range(GROUPS):
        for copy in loads[g]:
            copy.wait()
        lax.fori_loop(g * chunks, (g + 1) * chunks, factor, 0)
        swap(0, SF1, PF1, g).start()
        swap(1, SG, PG, g).start()

    def back_first(i, total):
        here = span(i)
        own_g = SG[here, :]
        e = 1.0 / (1.0 - own_g * PG[here, :])
        E[here, :] = e
        value = (SF1[here, :] + own_g * PF1[here, :]) * e
        ZP[order[-1], span(i, SUB), :] = value
        total = total + folded(value * R[order[-1], here, :])
        for k in range(depth - 2, -1, -1):
            l = order[k]
            value = ZP[l, span(i, SUB), :] + C[k, here, :] * INV[l, here, :] * value
            ZP[l, span(i, SUB), :] = value
            total = total + folded(value * R[l, here, :])
        return total

    zero = jnp.zeros((SUB, LANE), jnp.float32)
    b0 = zero
    for g in range(GROUPS):
        swap(0, SF1, PF1, g).wait_recv()
        swap(1, SG, PG, g).wait_recv()
        b0 = lax.fori_loop(g * chunks, (g + 1) * chunks, back_first, b0)

    def send_halos(n, field):
        inner = pl.ds(SUB, rows)
        for l in range(depth):
            row_send[n, 0, l] = field[l, pl.ds(SUB + rows - 1, 1), :]
            row_send[n, 1, l] = field[l, pl.ds(SUB, 1), :]
        col_send[n, 0] = pack_columns(lambda l: field[l, inner, cols - LANE:], LANE - 1)
        col_send[n, 1] = pack_columns(lambda l: field[l, inner, :LANE], 0)
        guarded(n, (0, 1), "start")

    def lateral(field, l, i):
        here = span(i)
        value = field[l, span(i, SUB), :]
        total = RC[l, span(i, SUB), :] * from_below(value, field[l, span(i, 2 * SUB), :])
        total = total + RU[l, here, :] * from_above(value, field[l, here, :])
        total = total + CC[l, here, :] * shift_left(value, 0.0)
        total = total + CL[l, here, :] * shift_right(value, 0.0)
        return value, total

    def apply_halos(n, target, sign, weights):
        guarded(n, (0, 1), "recv")
        tall = [unpacked(n, side) for side in range(2)]
        sums = [jnp.zeros((1, LANE), jnp.float32)] * len(weights)
        for l in range(depth):
            for side in range(2):
                at = 0 if side == 0 else rows - 1
                coupling = RU[l, pl.ds(0, 1), :] if side == 0 else RC[l, pl.ds(SUB + rows - 1, 1), :]
                term = coupling * row_recv[n, side, l]
                target[l, pl.ds(at, 1), :] = target[l, pl.ds(at, 1), :] + sign * term
                sums = [total + folded(term * weight(l, pl.ds(SUB + at, 1), pl.ds(0, cols)))
                        for total, weight in zip(sums, weights)]
            for side in range(2):
                block = pl.ds(0, LANE) if side == 0 else pl.ds(cols - LANE, LANE)
                coupling = CL[l, :, block] if side == 0 else CC[l, :, block]
                edge = lane_tall == (0 if side == 0 else LANE - 1)
                halo = jnp.broadcast_to(tall[side][:, l:l + 1], (rows, LANE))
                term = jnp.where(edge, coupling * halo, 0.0)
                target[l, :, block] = target[l, :, block] + sign * term
                sums = [total + jnp.sum(term * weight(l, pl.ds(SUB, rows), block), axis=0, keepdims=True)
                        for total, weight in zip(sums, weights)]
        return sums

    def image_first(i, total):
        for l in range(depth):
            value, around = lateral(ZP, l, i)
            W[l, span(i), :] = R[l, span(i), :] - around
            total = total + folded(value * around)
        return total

    def forward_second(i, total):
        here = span(i)
        before_f = None
        for k in range(depth):
            l = order[k]
            w = W[l, here, :]
            total = total + folded(ZP[l, span(i, SUB), :] * w)
            if k:
                w = w + C[k - 1, here, :] * before_f
            before_f = w * INV[l, here, :]
            YP[l, span(i, SUB), :] = before_f
        SF2[here, :] = before_f
        return total

    send_halos(1, ZP)
    s1 = lax.fori_loop(0, rows // SUB, image_first, zero)
    s1_edge, = apply_halos(1, W, -1.0, (lambda l, i, j: ZP[l, i, j],))

    g00 = zero
    for g in range(GROUPS):
        g00 = lax.fori_loop(g * chunks, (g + 1) * chunks, forward_second, g00)
        swap(2, SF2, PF2, g).start()

    def back_second(i, total):
        here = span(i)
        value = (SF2[here, :] + SG[here, :] * PF2[here, :]) * E[here, :]
        YP[order[-1], span(i, SUB), :] = value
        total = total + folded(value * W[order[-1], here, :])
        for k in range(depth - 2, -1, -1):
            l = order[k]
            value = YP[l, span(i, SUB), :] + C[k, here, :] * INV[l, here, :] * value
            YP[l, span(i, SUB), :] = value
            total = total + folded(value * W[l, here, :])
        return total

    g01 = zero
    for g in range(GROUPS):
        swap(2, SF2, PF2, g).wait_recv()
        g01 = lax.fori_loop(g * chunks, (g + 1) * chunks, back_second, g01)

    send_halos(2, YP)

    def image_second(i, total):
        here = span(i)
        for l in range(depth):
            value, around = lateral(YP, l, i)
            V[l, here, :] = around
            z = ZP[l, span(i, SUB), :]
            total = (total[0] + folded(value * (W[l, here, :] - around)),
                     total[1] + folded(z * around), total[2] + folded((z - value) * around))
        return total

    g11, q01, q11 = lax.fori_loop(0, rows // SUB, image_second, (zero, zero, zero))

    yy_edge, q01_edge, q11_edge = apply_halos(2, V, 1.0, (
        lambda l, i, j: YP[l, i, j],
        lambda l, i, j: ZP[l, i, j],
        lambda l, i, j: ZP[l, i, j] - YP[l, i, j]))

    parts = [jnp.sum(value, axis=0, keepdims=True) for value in (b0, g00, g01, g11, s1, q01, q11)]
    for n, edge in ((3, -yy_edge), (4, s1_edge), (5, q01_edge), (6, q11_edge)):
        parts[n] = parts[n] + edge
    partial = jnp.concatenate(parts + [jnp.zeros((1, LANE), jnp.float32)], axis=0)

    def all_sum(partial, stage_at, peers, me, count, buffer, send_sem, recv_sem):
        sums_send[stage_at] = partial
        buffer[me] = partial

        def copy(d, slot):
            return remote(sums_send.at[stage_at], buffer.at[slot], send_sem.at[d], recv_sem.at[slot], peers(d))

        for d in range(1, count):
            copy(d, me).start()
        for d in range(1, count):
            copy(d, lax.rem(me + count - d, count)).wait_recv()
        for d in range(1, count):
            copy(d, me).wait_send()
        total = buffer[0]
        for n in range(1, count):
            total = total + buffer[n]
        return total

    partial = all_sum(partial, 0, in_plane, mine, wide, sums_plane, plane_sum_send, plane_sum_recv)
    partial = all_sum(partial, 1, in_px, px, npx, sums_px, px_send_sem, px_recv_sem)
    flat = jnp.broadcast_to(jnp.sum(partial, axis=1, keepdims=True), (SUB, LANE))
    b0, g00, g01, g11, s1, q01, q11 = (flat[n:n + 1, :] / flat[1:2, :] for n in range(7))
    det_q = q11 - q01 * q01
    a_q = (b0 * q11 - q01 * s1) / det_q
    b_q = (s1 - q01 * b0) / det_q
    det_y = g11 - g01 * g01
    c1 = (1.0 - g01 * b0) / det_y
    c0 = (b0 * g11 - g01) / det_y
    take_q = q01 * q01 * g11 <= g01 * g01 * q11
    a = jnp.where(take_q, a_q, c0 + c1)
    b = jnp.where(take_q, b_q, -c1)

    def spread(value):
        return jnp.concatenate([value] * (cols // LANE), axis=1)

    coef_z[...] = spread(a + b)
    coef_y[...] = spread(-b)
    coef_w[...] = spread(a)
    coef_v[...] = spread(b)

    @pl.when(core == 0)
    def _():
        for copy in planes:
            copy.wait_send()

    guarded(0, (0,), "send")
    guarded(1, (0, 1), "send")
    guarded(2, (0, 1), "send")
    for g in range(GROUPS):
        swap(0, SF1, PF1, g).wait_send()
        swap(1, SG, PG, g).wait_send()
        swap(2, SF2, PF2, g).wait_send()


def shards(right_side, row_conduct, column_conduct, via_conduct, via_mask, ground_conduct):
    depth, rows, cols = right_side.shape
    npx, npy = lax.axis_size("px"), lax.axis_size("py")
    f32 = jnp.float32
    block = pltpu.VMEM((depth, rows, cols), f32)
    plane = pltpu.VMEM((rows, cols), f32)
    dma = pltpu.SemaphoreType.DMA
    scratch = [
        pltpu.VMEM((depth, rows + SUB, cols), f32), block, block,
        pltpu.VMEM((depth, rows, cols), jnp.int32), block, block, block, block, block,
        plane, pltpu.VMEM((rows, cols), jnp.int32), plane, plane, plane, plane, plane, plane, plane,
        pltpu.VMEM((depth, SUB, cols), f32), pltpu.VMEM((depth, rows, LANE), f32),
        pltpu.VMEM((3, 2, depth, 1, cols), f32), pltpu.VMEM((3, 2, depth, 1, cols), f32),
        pltpu.VMEM((3, 2, SUB, rows), f32), pltpu.VMEM((3, 2, SUB, rows), f32),
        pltpu.VMEM((depth, rows, LANE), f32),
        pltpu.VMEM((2, SUB, LANE), f32), pltpu.VMEM((2 * npy, SUB, LANE), f32),
        pltpu.VMEM((npx, SUB, LANE), f32),
        dma((GROUPS, 6)), dma((2,)), dma((2,)), dma((2,)), dma((3, GROUPS)), dma((3, GROUPS)),
        dma((3, 2)), dma((3, 2)), dma((3, 2)), dma((3, 2)),
        dma((2 * npy,)), dma((2 * npy,)), dma((npx,)), dma((npx,)),
    ]
    anywhere = pl.BlockSpec(memory_space=pl.ANY)
    padded = pltpu.VMEM((depth, rows + 2 * SUB, cols), f32)
    near = pl.BlockSpec(memory_space=pltpu.VMEM)
    row = pltpu.VMEM((1, cols), f32)
    z, y, w, v, r, coef_z, coef_y, coef_w, coef_v = pl.pallas_call(
        kernel,
        out_shape=(padded, padded, block, block, block, row, row, row, row),
        in_specs=[anywhere] * 6,
        out_specs=(near,) * 9,
        scratch_shapes=scratch,
        compiler_params=pltpu.CompilerParams(
            collective_id=0, has_side_effects=True, vmem_limit_bytes=VMEM_LIMIT),
        name="pcg",
    )(right_side, row_conduct, column_conduct, via_conduct, via_mask, ground_conduct)
    inner = slice(SUB, SUB + rows)
    return coef_z * z[:, inner, :] + coef_y * y[:, inner, :], r - coef_w * w - coef_v * v


def solution(mesh):
    spec = P("layer", "px", "py")
    return jax.shard_map(shards, mesh=mesh, in_specs=(spec,) * 6, out_specs=(spec, spec), check_vma=False)
```

```python
import jax
import jax.numpy as jnp
from jax import lax
from jax.experimental import pallas as pl
from jax.experimental.pallas import tpu as pltpu
from jax.sharding import PartitionSpec as P

GROUPS = 8
SUB = 8
LANE = 128
VMEM_LIMIT = 52 * 1024 * 1024


def kernel(
    r_hbm, rc_hbm, cc_hbm, via_hbm, mask_hbm, gr_hbm,
    ZP, YP, W, V, R, coef_z, coef_y, coef_w, coef_v,
    RC, CC, VI, MK, GR, RU, CL, C, INV,
    PV, PM, SF1, SG, SF2, PF1, PG, PF2, E,
    stage_row, stage_col, row_send, row_recv, col_send, col_recv, HL0,
    sums_send, sums_plane, sums_px,
    load_sem, stage_sem, plane_send_sem, plane_recv_sem, swap_send_sem, swap_recv_sem,
    row_send_sem, row_recv_sem, col_send_sem, col_recv_sem,
    plane_sum_send, plane_sum_recv, px_send_sem, px_recv_sem,
):
    depth, rows, cols = r_hbm.shape
    npx, npy = lax.axis_size("px"), lax.axis_size("py")
    core, px, py = lax.axis_index("layer"), lax.axis_index("px"), lax.axis_index("py")
    other = 1 - core
    size = rows // GROUPS
    chunks = size // SUB

    def remote(src, dst, send_sem, recv_sem, where):
        return pltpu.make_async_remote_copy(
            src_ref=src, dst_ref=dst, send_sem=send_sem, recv_sem=recv_sem,
            device_id=where, device_id_type=pl.DeviceIdType.MESH)

    stage = [
        pltpu.make_async_copy(rc_hbm.at[:, pl.ds(rows - SUB, SUB), :], stage_row, stage_sem.at[0]),
        pltpu.make_async_copy(cc_hbm.at[:, :, pl.ds(cols - LANE, LANE)], stage_col, stage_sem.at[1]),
    ]
    for copy in stage:
        copy.start()
    own_planes = [
        pltpu.make_async_copy(via_hbm.at[depth - 1], PV, plane_recv_sem.at[0]),
        pltpu.make_async_copy(mask_hbm.at[depth - 1], PM, plane_recv_sem.at[1]),
    ]

    @pl.when(core == 0)
    def _():
        for copy in own_planes:
            copy.start()

    loads = []
    for g in range(GROUPS):
        here = pl.ds(g * size, size)
        padded = pl.ds(SUB + g * size, size)
        pairs = ((rc_hbm, RC, padded), (cc_hbm, CC, here), (via_hbm, VI, here),
                 (mask_hbm, MK, here), (gr_hbm, GR, here), (r_hbm, R, here))
        group = [pltpu.make_async_copy(src.at[pl.ds(0, dst.shape[0]), here, :], dst.at[:, at, :], load_sem.at[g, n])
                 for n, (src, dst, at) in enumerate(pairs)]
        for copy in group:
            copy.start()
        loads.append(group)

    barrier = pltpu.get_barrier_semaphore()
    wide = 2 * npy
    mine = core * npy + py

    def in_plane(d):
        at = lax.rem(mine + d, wide)
        return {"layer": at // npy, "py": lax.rem(at, npy)}

    def in_px(d):
        return {"px": lax.rem(px + d, npx)}

    for peers, count in ((in_plane, wide), (in_px, npx)):
        for d in range(1, count):
            pl.semaphore_signal(barrier, inc=1, device_id=peers(d), device_id_type=pl.DeviceIdType.MESH)

    for field in (ZP, YP):
        field[:, pl.ds(0, SUB), :] = jnp.zeros((depth, SUB, cols), jnp.float32)
        field[:, pl.ds(SUB + rows, SUB), :] = jnp.zeros((depth, SUB, cols), jnp.float32)

    @pl.when(px == 0)
    def _():
        for n in range(3):
            row_recv[n, 0] = jnp.zeros((depth, 1, cols), jnp.float32)

    @pl.when(px == npx - 1)
    def _():
        for n in range(3):
            row_recv[n, 1] = jnp.zeros((depth, 1, cols), jnp.float32)

    @pl.when(py == 0)
    def _():
        for n in range(3):
            col_recv[n, 0] = jnp.zeros((SUB, rows), jnp.float32)

    @pl.when(py == npy - 1)
    def _():
        for n in range(3):
            col_recv[n, 1] = jnp.zeros((SUB, rows), jnp.float32)

    pl.semaphore_wait(barrier, wide + npx - 2)

    planes = [
        remote(PV, PV, plane_send_sem.at[0], plane_recv_sem.at[0], {"layer": other}),
        remote(PM, PM, plane_send_sem.at[1], plane_recv_sem.at[1], {"layer": other}),
    ]

    @pl.when(core == 0)
    def _():
        for copy in own_planes:
            copy.wait()
        for copy in planes:
            copy.start()

    lane = lax.broadcasted_iota(jnp.int32, (SUB, LANE), 1)
    sub = lax.broadcasted_iota(jnp.int32, (SUB, cols), 0)
    lane_tall = lax.broadcasted_iota(jnp.int32, (rows, LANE), 1)

    def row_copy(n, side):
        to = px + 1 if side == 0 else px - 1
        return remote(row_send.at[n, side], row_recv.at[n, side], row_send_sem.at[n, side],
                      row_recv_sem.at[n, side], {"px": to})

    def col_copy(n, side):
        to = py + 1 if side == 0 else py - 1
        return remote(col_send.at[n, side], col_recv.at[n, side], col_send_sem.at[n, side],
                      col_recv_sem.at[n, side], {"py": to})

    def guarded(n, sides, what):
        for side in sides:
            row_out = px < npx - 1 if side == 0 else px > 0
            col_out = py < npy - 1 if side == 0 else py > 0
            row_in = px > 0 if side == 0 else px < npx - 1
            col_in = py > 0 if side == 0 else py < npy - 1
            if what == "start":
                pl.when(col_out)(lambda s=side: col_copy(n, s).start())
                pl.when(row_out)(lambda s=side: row_copy(n, s).start())
            elif what == "recv":
                pl.when(row_in)(lambda s=side: row_copy(n, s).wait_recv())
                pl.when(col_in)(lambda s=side: col_copy(n, s).wait_recv())
            else:
                pl.when(row_out)(lambda s=side: row_copy(n, s).wait_send())
                pl.when(col_out)(lambda s=side: col_copy(n, s).wait_send())

    def pack_columns(tile_of, at):
        packed = jnp.zeros((rows, LANE), jnp.float32)
        for l in range(depth):
            column = jnp.broadcast_to(tile_of(l)[:, at:at + 1], (rows, LANE))
            packed = jnp.where(lane_tall == l, column, packed)
        return jnp.transpose(packed)[:SUB, :]

    def unpacked(n, side):
        return jnp.transpose(jnp.concatenate(
            [col_recv[n, side], jnp.zeros((LANE - SUB, rows), jnp.float32)], axis=0))

    for copy in stage:
        copy.wait()
    for l in range(depth):
        row_send[0, 0, l] = stage_row[l, SUB - 1:SUB, :]
    col_send[0, 0] = pack_columns(lambda l: stage_col[l], LANE - 1)
    guarded(0, (0,), "start")

    def shift_left(value, halo):
        rolled = pltpu.roll(value, cols - 1, 1)
        last = jnp.where(lane == LANE - 1, halo, rolled[:, cols - LANE:])
        return jnp.concatenate([rolled[:, :cols - LANE], last], axis=1)

    def shift_right(value, halo):
        rolled = pltpu.roll(value, 1, 1)
        first = jnp.where(lane == 0, halo, rolled[:, :LANE])
        return jnp.concatenate([first, rolled[:, LANE:]], axis=1)

    def from_above(value, before):
        return jnp.where(sub == 0, pltpu.roll(before, 1, 0), pltpu.roll(value, 1, 0))

    def from_below(value, after):
        return jnp.where(sub == SUB - 1, pltpu.roll(after, SUB - 1, 0), pltpu.roll(value, SUB - 1, 0))

    def folded(value):
        total = value[:, :LANE]
        for n in range(1, cols // LANE):
            total = total + value[:, n * LANE:(n + 1) * LANE]
        return total

    order = [k + core * (depth - 1 - 2 * k) for k in range(depth)]
    via_at = [k + core * (depth - 2 - 2 * k) for k in range(depth - 1)]

    def span(i, pad=0):
        return pl.ds(pl.multiple_of(i * SUB + pad, SUB), SUB)

    def swap(n, src, dst, g):
        here = pl.ds(g * size, size)
        return remote(src.at[here, :], dst.at[here, :], swap_send_sem.at[n, g], swap_recv_sem.at[n, g],
                      {"layer": other})

    guarded(0, (0,), "recv")
    tall = unpacked(0, 0)
    for l in range(depth):
        RC[l, pl.ds(SUB - 1, 1), :] = row_recv[0, 0, l]
        HL0[l] = jnp.broadcast_to(tall[:, l:l + 1], (rows, LANE))

    @pl.when(core == 1)
    def _():
        for copy in planes:
            copy.wait_recv()

    def factor(i, carry):
        here = span(i)
        before_c = before_g = before_f = None
        for k in range(depth):
            l = order[k]
            rc = RC[l, span(i, SUB), :]
            ru = from_above(rc, RC[l, here, :])
            cc = CC[l, here, :]
            cl = shift_right(cc, HL0[l, here, :])
            RU[l, here, :] = ru
            CL[l, here, :] = cl
            if k < depth - 1:
                c = VI[via_at[k], here, :] * MK[via_at[k], here, :].astype(jnp.float32)
            else:
                c = PV[here, :] * PM[here, :].astype(jnp.float32)
            diagonal = GR[l, here, :] + rc + ru + cc + cl + c
            r = R[l, here, :]
            if k:
                diagonal = (diagonal + before_c) - before_c * before_g
                r = r + before_c * before_f
            inverse = 1.0 / diagonal
            f = r * inverse
            g = c * inverse
            C[k, here, :] = c
            INV[l, here, :] = inverse
            ZP[l, span(i, SUB), :] = f
            before_c, before_g, before_f = c, g, f
        SF1[here, :] = before_f
        SG[here, :] = before_g
        return carry

    for g in range(GROUPS):
        for copy in loads[g]:
            copy.wait()
        lax.fori_loop(g * chunks, (g + 1) * chunks, factor, 0)
        swap(0, SF1, PF1, g).start()
        swap(1, SG, PG, g).start()

    def back_first(i, total):
        here = span(i)
        own_g = SG[here, :]
        e = 1.0 / (1.0 - own_g * PG[here, :])
        E[here, :] = e
        value = (SF1[here, :] + own_g * PF1[here, :]) * e
        ZP[order[-1], span(i, SUB), :] = value
        total = total + folded(value * R[order[-1], here, :])
        for k in range(depth - 2, -1, -1):
            l = order[k]
            value = ZP[l, span(i, SUB), :] + C[k, here, :] * INV[l, here, :] * value
            ZP[l, span(i, SUB), :] = value
            total = total + folded(value * R[l, here, :])
        return total

    zero = jnp.zeros((SUB, LANE), jnp.float32)
    b0 = zero
    for g in range(GROUPS):
        swap(0, SF1, PF1, g).wait_recv()
        swap(1, SG, PG, g).wait_recv()
        b0 = lax.fori_loop(g * chunks, (g + 1) * chunks, back_first, b0)

    def send_halos(n, field):
        inner = pl.ds(SUB, rows)
        for l in range(depth):
            row_send[n, 0, l] = field[l, pl.ds(SUB + rows - 1, 1), :]
            row_send[n, 1, l] = field[l, pl.ds(SUB, 1), :]
        col_send[n, 0] = pack_columns(lambda l: field[l, inner, cols - LANE:], LANE - 1)
        col_send[n, 1] = pack_columns(lambda l: field[l, inner, :LANE], 0)
        guarded(n, (0, 1), "start")

    def lateral(field, l, i):
        here = span(i)
        value = field[l, span(i, SUB), :]
        total = RC[l, span(i, SUB), :] * from_below(value, field[l, span(i, 2 * SUB), :])
        total = total + RU[l, here, :] * from_above(value, field[l, here, :])
        total = total + CC[l, here, :] * shift_left(value, 0.0)
        total = total + CL[l, here, :] * shift_right(value, 0.0)
        return value, total

    def apply_halos(n, target, sign, weights):
        guarded(n, (0, 1), "recv")
        tall = [unpacked(n, side) for side in range(2)]
        sums = [jnp.zeros((1, LANE), jnp.float32)] * len(weights)
        for l in range(depth):
            for side in range(2):
                at = 0 if side == 0 else rows - 1
                coupling = RU[l, pl.ds(0, 1), :] if side == 0 else RC[l, pl.ds(SUB + rows - 1, 1), :]
                term = coupling * row_recv[n, side, l]
                target[l, pl.ds(at, 1), :] = target[l, pl.ds(at, 1), :] + sign * term
                sums = [total + folded(term * weight(l, pl.ds(SUB + at, 1), pl.ds(0, cols)))
                        for total, weight in zip(sums, weights)]
            for side in range(2):
                block = pl.ds(0, LANE) if side == 0 else pl.ds(cols - LANE, LANE)
                coupling = CL[l, :, block] if side == 0 else CC[l, :, block]
                edge = lane_tall == (0 if side == 0 else LANE - 1)
                halo = jnp.broadcast_to(tall[side][:, l:l + 1], (rows, LANE))
                term = jnp.where(edge, coupling * halo, 0.0)
                target[l, :, block] = target[l, :, block] + sign * term
                sums = [total + jnp.sum(term * weight(l, pl.ds(SUB, rows), block), axis=0, keepdims=True)
                        for total, weight in zip(sums, weights)]
        return sums

    def image_first(i, total):
        for l in range(depth):
            value, around = lateral(ZP, l, i)
            W[l, span(i), :] = R[l, span(i), :] - around
            total = total + folded(value * around)
        return total

    def forward_second(i, total):
        here = span(i)
        before_f = None
        for k in range(depth):
            l = order[k]
            w = W[l, here, :]
            total = total + folded(ZP[l, span(i, SUB), :] * w)
            if k:
                w = w + C[k - 1, here, :] * before_f
            before_f = w * INV[l, here, :]
            YP[l, span(i, SUB), :] = before_f
        SF2[here, :] = before_f
        return total

    send_halos(1, ZP)
    s1 = lax.fori_loop(0, rows // SUB, image_first, zero)
    s1_edge, = apply_halos(1, W, -1.0, (lambda l, i, j: ZP[l, i, j],))

    g00 = zero
    for g in range(GROUPS):
        g00 = lax.fori_loop(g * chunks, (g + 1) * chunks, forward_second, g00)
        swap(2, SF2, PF2, g).start()

    def back_second(i, total):
        here = span(i)
        value = (SF2[here, :] + SG[here, :] * PF2[here, :]) * E[here, :]
        YP[order[-1], span(i, SUB), :] = value
        total = total + folded(value * W[order[-1], here, :])
        for k in range(depth - 2, -1, -1):
            l = order[k]
            value = YP[l, span(i, SUB), :] + C[k, here, :] * INV[l, here, :] * value
            YP[l, span(i, SUB), :] = value
            total = total + folded(value * W[l, here, :])
        return total

    g01 = zero
    for g in range(GROUPS):
        swap(2, SF2, PF2, g).wait_recv()
        g01 = lax.fori_loop(g * chunks, (g + 1) * chunks, back_second, g01)

    send_halos(2, YP)

    def image_second(i, total):
        here = span(i)
        for l in range(depth):
            value, around = lateral(YP, l, i)
            V[l, here, :] = around
            z = ZP[l, span(i, SUB), :]
            total = (total[0] + folded(value * (W[l, here, :] - around)),
                     total[1] + folded(z * around), total[2] + folded((z - value) * around))
        return total

    g11, q01, q11 = lax.fori_loop(0, rows // SUB, image_second, (zero, zero, zero))

    yy_edge, q01_edge, q11_edge = apply_halos(2, V, 1.0, (
        lambda l, i, j: YP[l, i, j],
        lambda l, i, j: ZP[l, i, j],
        lambda l, i, j: ZP[l, i, j] - YP[l, i, j]))

    parts = [jnp.sum(value, axis=0, keepdims=True) for value in (b0, g00, g01, g11, s1, q01, q11)]
    for n, edge in ((3, -yy_edge), (4, s1_edge), (5, q01_edge), (6, q11_edge)):
        parts[n] = parts[n] + edge
    partial = jnp.concatenate(parts + [jnp.zeros((1, LANE), jnp.float32)], axis=0)

    def all_sum(partial, stage_at, peers, me, count, buffer, send_sem, recv_sem):
        sums_send[stage_at] = partial
        buffer[me] = partial

        def copy(d, slot):
            return remote(sums_send.at[stage_at], buffer.at[slot], send_sem.at[d], recv_sem.at[slot], peers(d))

        for d in range(1, count):
            copy(d, me).start()
        for d in range(1, count):
            copy(d, lax.rem(me + count - d, count)).wait_recv()
        for d in range(1, count):
            copy(d, me).wait_send()
        total = buffer[0]
        for n in range(1, count):
            total = total + buffer[n]
        return total

    partial = all_sum(partial, 0, in_plane, mine, wide, sums_plane, plane_sum_send, plane_sum_recv)
    partial = all_sum(partial, 1, in_px, px, npx, sums_px, px_send_sem, px_recv_sem)
    flat = jnp.broadcast_to(jnp.sum(partial, axis=1, keepdims=True), (SUB, LANE))
    b0, g00, g01, g11, s1, q01, q11 = (flat[n:n + 1, :] / flat[1:2, :] for n in range(7))
    det_q = q11 - q01 * q01
    a_q = (b0 * q11 - q01 * s1) / det_q
    b_q = (s1 - q01 * b0) / det_q
    det_y = g11 - g01 * g01
    c1 = (1.0 - g01 * b0) / det_y
    c0 = (b0 * g11 - g01) / det_y
    take_q = q01 * q01 * g11 <= g01 * g01 * q11
    a = jnp.where(take_q, a_q, c0 + c1)
    b = jnp.where(take_q, b_q, -c1)

    def spread(value):
        return jnp.concatenate([value] * (cols // LANE), axis=1)

    coef_z[...] = spread(a + b)
    coef_y[...] = spread(-b)
    coef_w[...] = spread(a)
    coef_v[...] = spread(b)

    @pl.when(core == 0)
    def _():
        for copy in planes:
            copy.wait_send()

    guarded(0, (0,), "send")
    guarded(1, (0, 1), "send")
    guarded(2, (0, 1), "send")
    for g in range(GROUPS):
        swap(0, SF1, PF1, g).wait_send()
        swap(1, SG, PG, g).wait_send()
        swap(2, SF2, PF2, g).wait_send()


def shards(right_side, row_conduct, column_conduct, via_conduct, via_mask, ground_conduct):
    depth, rows, cols = right_side.shape
    npx, npy = lax.axis_size("px"), lax.axis_size("py")
    f32 = jnp.float32
    block = pltpu.VMEM((depth, rows, cols), f32)
    plane = pltpu.VMEM((rows, cols), f32)
    dma = pltpu.SemaphoreType.DMA
    scratch = [
        pltpu.VMEM((depth, rows + SUB, cols), f32), block, pltpu.VMEM((depth - 1, rows, cols), f32),
        pltpu.VMEM((depth - 1, rows, cols), jnp.int32), block, block, block, block, block,
        plane, pltpu.VMEM((rows, cols), jnp.int32), plane, plane, plane, plane, plane, plane, plane,
        pltpu.VMEM((depth, SUB, cols), f32), pltpu.VMEM((depth, rows, LANE), f32),
        pltpu.VMEM((3, 2, depth, 1, cols), f32), pltpu.VMEM((3, 2, depth, 1, cols), f32),
        pltpu.VMEM((3, 2, SUB, rows), f32), pltpu.VMEM((3, 2, SUB, rows), f32),
        pltpu.VMEM((depth, rows, LANE), f32),
        pltpu.VMEM((2, SUB, LANE), f32), pltpu.VMEM((2 * npy, SUB, LANE), f32),
        pltpu.VMEM((npx, SUB, LANE), f32),
        dma((GROUPS, 6)), dma((2,)), dma((2,)), dma((2,)), dma((3, GROUPS)), dma((3, GROUPS)),
        dma((3, 2)), dma((3, 2)), dma((3, 2)), dma((3, 2)),
        dma((2 * npy,)), dma((2 * npy,)), dma((npx,)), dma((npx,)),
    ]
    anywhere = pl.BlockSpec(memory_space=pl.ANY)
    padded = pltpu.VMEM((depth, rows + 2 * SUB, cols), f32)
    near = pl.BlockSpec(memory_space=pltpu.VMEM)
    row = pltpu.VMEM((1, cols), f32)
    z, y, w, v, r, coef_z, coef_y, coef_w, coef_v = pl.pallas_call(
        kernel,
        out_shape=(padded, padded, block, block, block, row, row, row, row),
        in_specs=[anywhere] * 6,
        out_specs=(near,) * 9,
        scratch_shapes=scratch,
        compiler_params=pltpu.CompilerParams(
            collective_id=0, has_side_effects=True, vmem_limit_bytes=VMEM_LIMIT),
        name="pcg",
    )(right_side, row_conduct, column_conduct, via_conduct, via_mask, ground_conduct)
    inner = slice(SUB, SUB + rows)
    return coef_z * z[:, inner, :] + coef_y * y[:, inner, :], r - coef_w * w - coef_v * v


def solution(mesh):
    spec = P("layer", "px", "py")
    return jax.shard_map(shards, mesh=mesh, in_specs=(spec,) * 6, out_specs=(spec, spec), check_vma=False)
```
